128 devices in a mesh: seq: 32 (over x, z, core), res: 4 (over y).
Axes of the slice: x: 4, y: 4, z: 4, core: 2. Of those that a mesh axis runs over, the one named last changes fastest.
Arguments:
- alignment: bfloat16 [512, 4, 512, 256], P('seq', 'res'), may hold values from -8 to 8
- gain_attn: float32 [256], replicated, may hold values from 0.1 to 1.9
- w_proj: bfloat16 [256, 4, 256], replicated, may hold values from -0.75 to 0.75
- w_out: bfloat16 [256, 256], replicated, may hold values from -0.375 to 0.375
- gain_head: float32 [256], replicated, may hold values from 0.1 to 1.9
- w_head: bfloat16 [256, 23], replicated, may hold values from -1 to 1
- masked: int32 [512, 4, 512], P('res', None, 'seq'), may hold values from 0 to 1
- labels: int32 [512, 4, 512], P('res', None, 'seq'), may hold values from 0 to 22
Outputs:
- updated: bfloat16 [512, 4, 512, 256], P('res', None, 'seq')
- masked_loss: float32 [], replicated
- mask_share: float32 [], replicated
The draws below stay inside these ranges and needn't reach their ends.
All inputs are finite; a program needn't handle non-finite values.
Results may differ from the reference program's by a relative error of at most 0.011.
Values may be sent and summed in bfloat16 or wider, within the bound.
A program may use at most 192 MiB of HBM per device.

```python
import math
import jax
import jax.numpy as jnp
from jax import lax

C = 256
HEADS = 8
HEAD_DIM = 32
CLASSES = 23
S = 512
RBLK = 4
RSEG = 512


def draw_alignment(key, part):
    row_key, scale_key = jax.random.split(jax.random.fold_in(key, 11), 2)
    deviation = jax.random.truncated_normal(row_key, -4.0, 4.0, (S, RBLK, RSEG, C), jnp.float32)
    scales = jnp.exp(jax.random.uniform(scale_key, (S, RBLK, RSEG, 1), jnp.float32, math.log(0.5), math.log(2.0)))
    return (deviation * scales).astype(jnp.bfloat16)


def draw_masked(key, part):
    ticket = jax.random.randint(jax.random.fold_in(key, 23), (S, RBLK, RSEG), 0, 1000, jnp.int32)
    limit = 50 + 100 * jnp.arange(RSEG, dtype=jnp.int32) // RSEG
    return (ticket < limit[None, None, :]).astype(jnp.int32)


def place_ends(values, stream_key, low, largest):
    longest = values.shape.index(max(values.shape))
    spots = []
    for shift in (0, 1):
        where = [jax.random.randint(jax.random.fold_in(stream_key, axis), (), 0, length) for axis, length in enumerate(values.shape)]
        where[longest] = (where[longest] + shift) % values.shape[longest]
        spots.append(tuple(where))
    return values.at[spots[0]].set(low).at[spots[1]].set(largest)


def scatter_about(own_key, shape, scale, reach, kind=jnp.bfloat16):
    return jnp.clip(scale * jax.random.normal(own_key, shape, jnp.float32), -reach, reach).astype(kind)


def setup_inputs(seed: int = 0) -> dict:
    arg_keys = jax.random.split(jax.random.key(seed), 9)
    return {
        "alignment": draw_alignment(jax.random.fold_in(arg_keys[8], 71), 0),
        "gain_attn": jnp.clip(1.0 + 0.18 * jax.random.normal(arg_keys[1], (C,), jnp.float32), 0.1, 1.9),
        "w_proj": scatter_about(arg_keys[2], (C, 4, C), (C // 4) ** -0.5, 0.75),
        "w_out": scatter_about(arg_keys[3], (C, C), C ** -0.5, 0.375),
        "gain_head": jnp.clip(1.0 + 0.18 * jax.random.normal(arg_keys[4], (C,), jnp.float32), 0.1, 1.9),
        "w_head": scatter_about(arg_keys[5], (C, CLASSES), (C // 9) ** -0.5, 1.0),
        "masked": draw_masked(jax.random.fold_in(arg_keys[8], 71), 0),
        "labels": place_ends(jax.random.randint(arg_keys[7], (S, RBLK, RSEG), 0, CLASSES), jax.random.fold_in(arg_keys[7], 1), 0, CLASSES - 1).astype(jnp.int32),
    }


def normalize(values, gain):
    mean = lax.optimization_barrier(jnp.mean(values, axis=-1, keepdims=True))
    centred = values - mean
    spread = lax.optimization_barrier(jnp.mean(centred * centred, axis=-1, keepdims=True))
    return centred * lax.rsqrt(spread + 1e-05) * gain

def column_update(column_rows, gain_attn, w_proj, w_out):
    normed = normalize(column_rows.astype(jnp.float32), gain_attn).astype(jnp.bfloat16)
    projected = jnp.dot(normed, w_proj.reshape(C, 4 * C), preferred_element_type=jnp.float32).astype(jnp.bfloat16)
    projected = lax.optimization_barrier(projected).astype(jnp.float32).reshape(S, 4, HEADS, HEAD_DIM)
    queries = projected[:, 0]
    keys_all = projected[:, 1]
    values_all = projected[:, 2]
    gates = projected[:, 3]
    scores = jnp.einsum('shd,thd->hst', queries, keys_all) * HEAD_DIM ** (-0.5)
    probs = jnp.exp(scores)
    totals = lax.optimization_barrier(jnp.sum(probs, axis=2))
    rounded = lax.optimization_barrier(probs.astype(jnp.bfloat16)).astype(jnp.float32)
    weighted = jnp.einsum('hst,thd->shd', rounded, values_all)
    attended = weighted / totals.T[:, :, None]
    gated = (attended * jax.nn.sigmoid(gates)).reshape(S, C).astype(jnp.bfloat16)
    result = column_rows.astype(jnp.float32) + jnp.dot(gated, w_out, preferred_element_type=jnp.float32)
    return result.astype(jnp.bfloat16)

def reference(alignment, gain_attn, w_proj, w_out, gain_head, w_head, masked, labels):
    columns = jnp.transpose(alignment.reshape(S, RBLK * RSEG, C), (1, 0, 2))
    updated_cols = lax.map(lambda column_rows: column_update(column_rows, gain_attn, w_proj, w_out), columns)
    updated = jnp.transpose(updated_cols, (1, 0, 2)).reshape(S, RBLK, RSEG, C)
    flat_out = updated.reshape(-1, C)
    head_in = normalize(flat_out.astype(jnp.float32), gain_head).astype(jnp.bfloat16)
    logits = jnp.dot(head_in, w_head, preferred_element_type=jnp.float32)
    log_total = jnp.log(lax.optimization_barrier(jnp.sum(jnp.exp(logits), axis=1)))
    classes = jnp.arange(CLASSES, dtype=jnp.int32)[None, :]
    picked = lax.optimization_barrier(jnp.sum(jnp.where(classes == labels.reshape(-1, 1), logits, 0.0), axis=1))
    errors = log_total - picked
    weights = masked.reshape(-1).astype(jnp.float32)
    loss_sum = jnp.sum(errors * weights)
    mask_count = jnp.sum(weights)
    masked_loss = loss_sum / (1.0 + mask_count)
    mask_share = mask_count / (S * RBLK * RSEG)
    return (updated, masked_loss, mask_share)
```

```python
import functools
import math

import jax
import jax.numpy as jnp
from jax import lax
from jax.experimental import pallas as pl
from jax.experimental.pallas import tpu as pltpu
from jax.sharding import Mesh
from jax.sharding import PartitionSpec as P

HEADS = 8
HEAD_DIM = 32
CLASSES = 23
C = 256
NSEQ = 32
NRES = 4
ROWS = 16
S = 512
COLS = 16
CHUNK = 2
CHUNKS = COLS // CHUNK
VAUG = 48
LPAD = 32
AXES = ("seq_0", "seq_1", "seq_2", "res")
SEQ = AXES[:3]
MESH = pl.DeviceIdType.MESH
BF = jnp.bfloat16
F32 = jnp.float32
QSCALE = HEAD_DIM ** (-0.5) * math.log2(math.e)


def seq_coords(index):
    return index // 8, (index // 2) % 4, index % 2


def swap_matrix(outer, inner):
    n = outer * inner
    row = lax.broadcasted_iota(jnp.int32, (n, n), 0)
    col = lax.broadcasted_iota(jnp.int32, (n, n), 1)
    source = (row % outer) * inner + row // outer
    return jnp.where(col == source, 1.0, 0.0).astype(BF)


def normed_rows(values, gain):
    mean = jnp.mean(values, axis=-1, keepdims=True)
    centred = values - mean
    spread = jnp.mean(centred * centred, axis=-1, keepdims=True)
    return (centred * lax.rsqrt(spread + 1e-05) * gain).astype(BF)


def dot(a, b, dims=((1,), (0,))):
    return lax.dot_general(a, b, (dims, ((), ())), preferred_element_type=F32)


def exchange_kernel(
    align_hbm, codes_ref, gain_attn, w_k, w_qvg, w_out, gain_head, w_head,
    out_hbm, stats_ref,
    align_v, sendbuf, recv, outbuf, codes_r, qz, va, gt, gated_t, k_nat, perm, acc, st_y, st_s,
    load_sem, send_sem, recv_sem, ysend_sem, yrecv_sem, own_sem, code_sem, csend_sem, ar_sem, ars_sem,
):
    x, z, core, y = (lax.axis_index(a) for a in AXES)
    me = (x * 4 + z) * 2 + core

    def seq_device(i):
        dx, dz, dc = seq_coords(lax.rem(me + i, NSEQ))
        return (dx, dz, dc, y)

    def res_device(k):
        return (x, z, core, lax.rem(y + k, NRES))

    loads = [
        pltpu.make_async_copy(
            align_hbm.at[:, 0, pl.ds(128 * j, 128)], align_v.at[:, pl.ds(128 * j, 128)], load_sem.at[j]
        )
        for j in range(4)
    ]
    for load in loads:
        load.start()

    barrier = pltpu.get_barrier_semaphore()

    @pl.loop(1, NSEQ)
    def _(i):
        pl.semaphore_signal(barrier, inc=1, device_id=seq_device(i), device_id_type=MESH)

    for k in range(1, NRES):
        pl.semaphore_signal(barrier, inc=1, device_id=res_device(k), device_id_type=MESH)

    perm[...] = swap_matrix(ROWS, COLS)
    qz[...] = jnp.zeros_like(qz)
    va[...] = jnp.ones_like(va)
    acc[...] = jnp.zeros_like(acc)
    for j in range(4):
        loads[j].wait()

        @pl.loop(8 * j, 8 * j + 8)
        def _(d):
            block = align_v[:, pl.ds(pl.multiple_of(d * COLS, COLS), COLS)].reshape(ROWS * COLS, C)
            moved = dot(perm[...], block).astype(BF)
            sendbuf[d] = moved.reshape(COLS, ROWS, C)

    for m in range(CHUNKS):
        recv[m, me] = sendbuf[me, pl.ds(CHUNK * m, CHUNK)]
    codes_r[y] = codes_ref[y]

    pl.semaphore_wait(barrier, NSEQ - 1 + NRES - 1)

    for k in range(1, NRES):
        pltpu.make_async_remote_copy(
            codes_ref.at[lax.rem(y + k, NRES)], codes_r.at[y], csend_sem, code_sem,
            device_id=res_device(k), device_id_type=MESH,
        ).start()

    @pl.loop(0, CHUNKS)
    def _(m):
        @pl.loop(1, NSEQ)
        def _(i):
            pltpu.make_async_remote_copy(
                sendbuf.at[lax.rem(me + i, NSEQ), pl.ds(m * CHUNK, CHUNK)], recv.at[m, me],
                send_sem, recv_sem.at[m], device_id=seq_device(i), device_id_type=MESH,
            ).start()

    pltpu.make_async_copy(codes_r.at[pl.ds(0, 3)], codes_r.at[pl.ds(0, 3)], code_sem).wait()
    count = jnp.sum((codes_r[...] >= 32).astype(F32), axis=0)
    acc[pl.ds(8, 8)] = count[:8] + count[8:]

    @pl.loop(0, COLS)
    def _(c):
        m = c // CHUNK
        j = c % CHUNK

        @pl.when(j == 0)
        def _():
            span = recv.at[m, pl.ds(0, NSEQ - 1)]
            pltpu.make_async_copy(span, span, recv_sem.at[m]).wait()

        rows = recv[m, :, j].reshape(S, C).astype(F32)
        normed = normed_rows(rows, gain_attn[...])
        k_nat[...] = dot(normed, w_k[...]).astype(BF)
        q_t = dot(w_qvg[pl.ds(0, C)], normed, ((1,), (1,)))
        q_t = (q_t * QSCALE).astype(BF)
        v_t = dot(w_qvg[pl.ds(C, C)], normed, ((1,), (1,))).astype(BF)
        for h in range(HEADS):
            part = slice(HEAD_DIM * h, HEAD_DIM * (h + 1))
            qz[h, part] = q_t[part]
            va[h, :HEAD_DIM] = v_t[part]
        gt[...] = dot(w_qvg[pl.ds(2 * C, C)], normed, ((1,), (1,))).astype(BF)

        @pl.loop(0, HEADS)
        def _(h):
            scores = dot(k_nat[...], qz[h])
            probs = jnp.exp2(scores).astype(BF)
            weighted = dot(va[h], probs)
            span = pl.ds(pl.multiple_of(h * HEAD_DIM, HEAD_DIM), HEAD_DIM)
            gate = jax.nn.sigmoid(gt[span].astype(F32))
            gated = weighted[:HEAD_DIM] / weighted[HEAD_DIM : HEAD_DIM + 1] * gate
            gated_t[span] = gated.astype(BF)

        added = dot(gated_t[...], w_out[...], ((0,), (0,)))
        updated = (recv[m, :, j].reshape(S, C).astype(F32) + added).astype(BF)
        outbuf[c] = updated

        for k in range(1, NRES):
            dst = lax.rem(y + k, NRES)
            pltpu.make_async_remote_copy(
                outbuf.at[c, pl.ds(pl.multiple_of(dst * 128, 128), 128)], out_hbm.at[y, c],
                ysend_sem, yrecv_sem, device_id=res_device(k), device_id_type=MESH,
            ).start()
        pltpu.make_async_copy(
            outbuf.at[c, pl.ds(pl.multiple_of(y * 128, 128), 128)], out_hbm.at[y, c], own_sem
        ).start()

        head_in = normed_rows(updated.astype(F32), gain_head[...])
        logits = dot(w_head[...], head_in, ((1,), (1,)))
        log_total = jnp.log(jnp.sum(jnp.exp(logits[:CLASSES]), axis=0, keepdims=True))
        classes = lax.broadcasted_iota(jnp.int32, (LPAD, 128), 0)
        for i in range(NRES):
            lanes = slice(128 * i, 128 * (i + 1))
            code = codes_r[i, pl.ds(c, 1)]
            picked = jnp.sum(
                jnp.where(classes == (code & 31), logits[:, lanes], 0.0), axis=0, keepdims=True
            )
            error = log_total[:, lanes] - picked
            acc[pl.ds(0, 1)] += jnp.where(code >= 32, error, 0.0)

    total_count = jnp.sum(acc[pl.ds(8, 8)], axis=0, keepdims=True)
    first = lax.broadcasted_iota(jnp.int32, (8, 128), 0) == 0
    st_y[y] = jnp.where(first, acc[pl.ds(0, 1)], total_count)
    for k in range(1, NRES):
        pltpu.make_async_remote_copy(
            st_y.at[y], st_y.at[y], ars_sem.at[0], ar_sem.at[0],
            device_id=res_device(k), device_id_type=MESH,
        ).start()
    pltpu.make_async_copy(st_y.at[pl.ds(0, 3)], st_y.at[pl.ds(0, 3)], ar_sem.at[0]).wait()
    st_s[me] = (st_y[0] + st_y[1]) + (st_y[2] + st_y[3])

    @pl.loop(1, NSEQ)
    def _(i):
        pltpu.make_async_remote_copy(
            st_s.at[me], st_s.at[me], ars_sem.at[1], ar_sem.at[1],
            device_id=seq_device(i), device_id_type=MESH,
        ).start()

    pltpu.make_async_copy(st_s.at[pl.ds(0, NSEQ - 1)], st_s.at[pl.ds(0, NSEQ - 1)], ar_sem.at[1]).wait()
    sums = jnp.sum(jnp.sum(st_s[...], axis=0), axis=1, keepdims=True)
    stats_ref[...] = jnp.broadcast_to(sums, (8, 128))

    pltpu.make_async_copy(st_y.at[pl.ds(0, 3)], st_y.at[pl.ds(0, 3)], ars_sem.at[0]).wait()
    pltpu.make_async_copy(st_s.at[pl.ds(0, NSEQ - 1)], st_s.at[pl.ds(0, NSEQ - 1)], ars_sem.at[1]).wait()
    pltpu.make_async_copy(codes_r.at[pl.ds(0, 3)], codes_r.at[pl.ds(0, 3)], csend_sem).wait()
    sent = sendbuf.at[pl.ds(0, NSEQ - 1)]
    pltpu.make_async_copy(sent, sent, send_sem).wait()
    pltpu.make_async_copy(out_hbm.at[0], out_hbm.at[0], own_sem).wait()
    three = out_hbm.at[pl.ds(0, 3)]
    pltpu.make_async_copy(three, three, ysend_sem).wait()
    pltpu.make_async_copy(three, three, yrecv_sem).wait()


def finish_kernel(part_ref, stats_ref, out_ref, loss_ref, share_ref):
    perm = swap_matrix(COLS, ROWS)
    for b in range(NRES):
        block = part_ref[b].reshape(COLS * ROWS, C)
        out_ref[:, b] = dot(perm, block).astype(BF).reshape(ROWS, COLS, C)
    loss_sum = stats_ref[0, 0]
    mask_count = stats_ref[1, 0]
    loss_ref[0, 0] = loss_sum / (1.0 + mask_count)
    share_ref[0, 0] = mask_count * (1.0 / 1048576)


def on_device(alignment, gain_attn, w_proj, w_out, gain_head, w_head, masked, labels):
    codes = jnp.transpose(labels + 32 * masked, (1, 2, 0))
    w_k = w_proj[:, 1]
    w_qvg = jnp.concatenate([w_proj[:, i].T for i in (0, 2, 3)], axis=0)
    w_head_t = jnp.pad(w_head.T, ((0, LPAD - CLASSES), (0, 0)))
    vmem = pl.BlockSpec(memory_space=pltpu.VMEM)
    hbm = pl.BlockSpec(memory_space=pl.ANY)
    dma = pltpu.SemaphoreType.DMA
    parts, stats = pl.pallas_call(
        exchange_kernel,
        out_shape=(
            jax.ShapeDtypeStruct((NRES, COLS, 128, C), BF),
            jax.ShapeDtypeStruct((8, 128), F32),
        ),
        in_specs=[hbm] + [vmem] * 7,
        out_specs=(hbm, vmem),
        scratch_shapes=[
            pltpu.VMEM((ROWS, S, C), BF),
            pltpu.VMEM((NSEQ, COLS, ROWS, C), BF),
            pltpu.VMEM((CHUNKS, NSEQ, CHUNK, ROWS, C), BF),
            pltpu.VMEM((COLS, S, C), BF),
            pltpu.VMEM((NRES, COLS, 128), jnp.int32),
            pltpu.VMEM((HEADS, C, S), BF),
            pltpu.VMEM((HEADS, VAUG, S), BF),
            pltpu.VMEM((C, S), BF),
            pltpu.VMEM((C, S), BF),
            pltpu.VMEM((S, C), BF),
            pltpu.VMEM((C, C), BF),
            pltpu.VMEM((16, 128), F32),
            pltpu.VMEM((NRES, 8, 128), F32),
            pltpu.VMEM((NSEQ, 8, 128), F32),
            dma((4,)), dma, dma((CHUNKS,)), dma, dma, dma, dma, dma, dma((2,)), dma((2,)),
        ],
        compiler_params=pltpu.CompilerParams(
            collective_id=0, has_side_effects=True, vmem_limit_bytes=60 * 2**20
        ),
        name="exchange",
    )(
        alignment, codes, gain_attn.reshape(1, C), w_k, w_qvg, w_out, gain_head.reshape(1, C), w_head_t,
    )
    smem = pl.BlockSpec(memory_space=pltpu.SMEM)
    updated, loss, share = pl.pallas_call(
        finish_kernel,
        grid=(128 // ROWS,),
        out_shape=(
            jax.ShapeDtypeStruct((128, NRES, COLS, C), BF),
            jax.ShapeDtypeStruct((1, 1), F32),
            jax.ShapeDtypeStruct((1, 1), F32),
        ),
        in_specs=[pl.BlockSpec((NRES, COLS, ROWS, C), lambda r: (0, 0, r, 0)), smem],
        out_specs=(pl.BlockSpec((ROWS, NRES, COLS, C), lambda r: (r, 0, 0, 0)), smem, smem),
        name="finish",
    )(parts, stats)
    return updated, loss.reshape(()), share.reshape(())


def solution(mesh):
    split = Mesh(mesh.devices.reshape(4, 4, 2, mesh.shape["res"]), AXES)
    return jax.shard_map(
        on_device,
        mesh=split,
        in_specs=(
            P(SEQ, "res", None, None), P(), P(), P(), P(), P(),
            P("res", None, SEQ), P("res", None, SEQ),
        ),
        out_specs=(P("res", None, SEQ, None), P(), P()),
        check_vma=False,
    )
```

```python
import math

import jax
import jax.numpy as jnp
from jax import lax
from jax.experimental import pallas as pl
from jax.experimental.pallas import tpu as pltpu
from jax.sharding import Mesh
from jax.sharding import PartitionSpec as P

HEADS = 8
HEAD_DIM = 32
CLASSES = 23
C = 256
NSEQ = 32
NRES = 4
ROWS = 16
S = 512
COLS = 16
VAUG = 48
LPAD = 32
VMEM_LIMIT = 48 * 2**20
AXES = ("seq_0", "seq_1", "seq_2", "res")
SEQ = AXES[:3]
MESH = pl.DeviceIdType.MESH
BF = jnp.bfloat16
F32 = jnp.float32
QSCALE = HEAD_DIM ** (-0.5) * math.log2(math.e)


def normed_rows(values, gain):
    mean = jnp.mean(values, axis=-1, keepdims=True)
    centred = values - mean
    spread = jnp.mean(centred * centred, axis=-1, keepdims=True)
    return (centred * lax.rsqrt(spread + 1e-05) * gain).astype(BF)


def dot(a, b, dims=((1,), (0,))):
    return lax.dot_general(a, b, (dims, ((), ())), preferred_element_type=F32)


def exchange_kernel(
    align_hbm, w_proj_hbm, w_out_ref, w_head_hbm, gains_a_hbm, gains_h_hbm, masked_hbm, labels_hbm,
    out_ref, stats_ref,
    align_v, sendbuf, recv, outbuf, codes, codes_r, w_proj_v, w_k, w_qvg, w_out, w_head_v, w_head,
    gain_attn, gain_head, masked_v, labels_v, qz, va, sg, gated_t, k_nat, sb, nm, hi, acc, st_y, st_s,
    load_sem, small_sem, send_sem, recv_sem, ysend_sem, yrecv_sem, code_sem, csend_sem, ar_sem, ars_sem,
):
    x, z, core, y = (lax.axis_index(a) for a in AXES)
    me = (x * 4 + z) * 2 + core

    at_x = [lax.rem(x + d, 4) for d in range(4)]
    at_z = [lax.rem(z + d, 4) for d in range(4)]
    at_core = [core, 1 - core]
    at_y = [lax.rem(y + d, NRES) for d in range(NRES)]

    def seq_device(i):
        return (at_x[i // 8], at_z[i // 2 % 4], at_core[i % 2], y)

    def seq_index(i):
        return (at_x[i // 8] * 4 + at_z[i // 2 % 4]) * 2 + at_core[i % 2]

    def res_device(k):
        return (x, z, core, at_y[k])

    barrier = pltpu.get_barrier_semaphore()

    for i in range(1, NSEQ):
        pl.semaphore_signal(barrier, inc=1, device_id=seq_device(i), device_id_type=MESH)

    for k in range(1, NRES):
        pl.semaphore_signal(barrier, inc=1, device_id=res_device(k), device_id_type=MESH)

    loads = [
        pltpu.make_async_copy(
            align_hbm.at[:, 0, pl.ds(128 * j, 128)], align_v.at[:, pl.ds(128 * j, 128)], load_sem.at[j]
        )
        for j in range(4)
    ]
    small = [
        pltpu.make_async_copy(src, dst, small_sem.at[n])
        for n, (src, dst) in enumerate(
            (
                (masked_hbm, masked_v), (labels_hbm, labels_v), (w_proj_hbm, w_proj_v),
                (w_out_ref, w_out), (w_head_hbm, w_head_v),
                (gains_a_hbm, gain_attn), (gains_h_hbm, gain_head),
            )
        )
    ]
    for copy in loads + small:
        copy.start()

    for j in range(4):
        loads[j].wait()

        @pl.loop(0, 2)
        def _(g):
            for u in range(4):
                d = 8 * j + 4 * g + u
                block = align_v[:, pl.ds(pl.multiple_of(d * COLS, COLS), COLS)]
                sendbuf[d] = jnp.swapaxes(block, 0, 1)

    recv[:, me] = sendbuf[me]

    for copy in small:
        copy.wait()
    codes[...] = labels_v[...] + 32 * masked_v[...]
    codes_r[y] = codes[y]

    pl.semaphore_wait(barrier, NSEQ - 1 + NRES - 1)

    for k in range(1, NRES):
        pltpu.make_async_remote_copy(
            codes.at[lax.rem(y + k, NRES)], codes_r.at[y], csend_sem, code_sem,
            device_id=res_device(k), device_id_type=MESH,
        ).start()

    @pl.loop(0, COLS)
    def _(c):
        for i in range(1, NSEQ):
            pltpu.make_async_remote_copy(
                sendbuf.at[seq_index(i), c], recv.at[c, me],
                send_sem, recv_sem.at[c], device_id=seq_device(i), device_id_type=MESH,
            ).start()

    for n, i in enumerate((0, 2, 3)):
        w_qvg[pl.ds(C * n, C)] = w_proj_v[:, i].astype(F32).T.astype(BF)
    w_k[...] = w_proj_v[:, 1]
    w_head[...] = jnp.zeros_like(w_head)
    w_head[:CLASSES] = w_head_v[...]
    gated_t[...] = jnp.zeros_like(gated_t)
    acc[...] = jnp.zeros_like(acc)
    for p in range(2):
        qz[p] = jnp.zeros((HEADS, C, S), BF)
        va[p] = jnp.ones((HEADS, VAUG, S), BF)

    pltpu.make_async_copy(codes_r.at[pl.ds(0, 3)], codes_r.at[pl.ds(0, 3)], code_sem).wait()
    count = jnp.sum((codes_r[...] >= 32).astype(F32), axis=0)
    acc[pl.ds(8, 8)] = count[:8] + count[8:]

    def arrived(c):
        span = recv.at[c, pl.ds(0, NSEQ - 1)]
        pltpu.make_async_copy(span, span, recv_sem.at[c]).wait()

    def rows(c, start, n):
        return recv[c, pl.ds(start // ROWS, n // ROWS)].reshape(n, C).astype(F32)

    def before(c, p):
        def norm(start):
            def run():
                nm[pl.ds(start, 128)] = normed_rows(rows(c, start, 128), gain_attn[...])
            return run

        def keys():
            k_nat[p] = dot(nm[...], w_k[...]).astype(BF)

        def queries():
            q_t = (dot(w_qvg[pl.ds(0, C)], nm[...], ((1,), (1,))) * QSCALE).astype(BF)
            for h in range(HEADS):
                part = slice(HEAD_DIM * h, HEAD_DIM * (h + 1))
                qz[p, h, part] = q_t[part]

        def values():
            v_t = dot(w_qvg[pl.ds(C, C)], nm[...], ((1,), (1,))).astype(BF)
            for h in range(HEADS):
                va[p, h, :HEAD_DIM] = v_t[HEAD_DIM * h : HEAD_DIM * (h + 1)]

        def gates():
            g_t = dot(w_qvg[pl.ds(2 * C, C)], nm[...], ((1,), (1,))).astype(BF).astype(F32)
            sg[p] = 0.5 * jnp.tanh(0.5 * g_t) + 0.5

        return [norm(0), norm(128), norm(256), norm(384), keys, queries, values, gates]

    def after(c, p, live):
        def project(start):
            def run():
                added = dot(gated_t[p, :, start : start + 256], w_out[...], ((0,), (0,)))
                outbuf[c, pl.ds(start, 256)] = (rows(c, start, 256) + added).astype(BF)
            return run

        def norm(start):
            def run():
                hi[pl.ds(start, 256)] = normed_rows(outbuf[c, pl.ds(start, 256)].astype(F32), gain_head[...])
            return run

        def loss():
            logits = dot(w_head[...], hi[...], ((1,), (1,)))
            log_total = jnp.log(jnp.sum(jnp.exp(logits[:CLASSES]), axis=0, keepdims=True))
            classes = lax.broadcasted_iota(jnp.int32, (LPAD, 128), 0)
            total = jnp.zeros((1, 128), F32)
            for i in range(NRES):
                lanes = slice(128 * i, 128 * (i + 1))
                code = codes_r[i, pl.ds(c, 1)]
                picked = jnp.sum(
                    jnp.where(classes == (code & 31), logits[:, lanes], 0.0), axis=0, keepdims=True
                )
                total += jnp.where(code >= 32, log_total[:, lanes] - picked, 0.0)
            if live is not None:
                total = jnp.where(live, total, 0.0)
            acc[pl.ds(0, 1)] += total

        return [project(0), project(256), norm(0), norm(256), loss]

    def send_out(c):
        for k in range(1, NRES):
            dst = lax.rem(y + k, NRES)
            pltpu.make_async_remote_copy(
                outbuf.at[c, pl.ds(pl.multiple_of(dst * 128, 128), 128)], out_ref.at[y, c],
                ysend_sem, yrecv_sem, device_id=res_device(k), device_id_type=MESH,
            ).start()
        out_ref[y, c] = outbuf[c, pl.ds(pl.multiple_of(y * 128, 128), 128)]

    def score(p, h):
        sb[h % 2] = dot(k_nat[p], qz[p, h])

    def attend(p, h):
        weighted = dot(va[p, h], jnp.exp2(sb[h % 2]).astype(BF))
        part = slice(HEAD_DIM * h, HEAD_DIM * (h + 1))
        inverse = 1.0 / weighted[HEAD_DIM : HEAD_DIM + 1]
        gated_t[p, part] = (weighted[:HEAD_DIM] * inverse * sg[p, part]).astype(BF)

    def body(c, p, following, live):
        slots = [[] for _ in range(HEADS)]
        if following is not None:
            arrived(following)
            for slot, piece in enumerate(before(following, 1 - p)):
                slots[slot].append(piece)
        last = c - 1 if live is None else jnp.maximum(c - 1, 0)
        for slot, piece in zip((0, 1, 3, 4, 6), after(last, 1 - p, live)):
            slots[slot].append(piece)
        for h in range(HEADS):
            if h + 1 < HEADS:
                score(p, h + 1)
            for piece in slots[h]:
                piece()
            if h + 1 == HEADS and following is not None:
                score(1 - p, 0)
            attend(p, h)
        if live is None:
            send_out(last)
        else:
            @pl.when(live)
            def _():
                send_out(last)

    arrived(0)
    for piece in before(0, 0):
        piece()
    score(0, 0)

    @pl.loop(0, COLS // 2 - 1)
    def _(i):
        body(2 * i, 0, 2 * i + 1, i > 0)
        body(2 * i + 1, 1, 2 * i + 2, None)

    body(COLS - 2, 0, COLS - 1, None)
    body(COLS - 1, 1, None, None)
    final = after(COLS - 1, 1, None)
    final[0]()
    final[1]()
    send_out(COLS - 1)
    for piece in final[2:]:
        piece()

    total_count = jnp.sum(acc[pl.ds(8, 8)], axis=0, keepdims=True)
    first = lax.broadcasted_iota(jnp.int32, (8, 128), 0) == 0
    st_y[y] = jnp.where(first, acc[pl.ds(0, 1)], total_count)
    for k in range(1, NRES):
        pltpu.make_async_remote_copy(
            st_y.at[y], st_y.at[y], ars_sem.at[0], ar_sem.at[0],
            device_id=res_device(k), device_id_type=MESH,
        ).start()
    pltpu.make_async_copy(st_y.at[pl.ds(0, 3)], st_y.at[pl.ds(0, 3)], ar_sem.at[0]).wait()
    st_s[me] = (st_y[0] + st_y[1]) + (st_y[2] + st_y[3])

    for i in range(1, NSEQ):
        pltpu.make_async_remote_copy(
            st_s.at[me], st_s.at[me], ars_sem.at[1], ar_sem.at[1],
            device_id=seq_device(i), device_id_type=MESH,
        ).start()

    pltpu.make_async_copy(st_s.at[pl.ds(0, NSEQ - 1)], st_s.at[pl.ds(0, NSEQ - 1)], ar_sem.at[1]).wait()
    sums = jnp.sum(jnp.sum(st_s[...], axis=0), axis=1, keepdims=True)
    stats_ref[...] = jnp.broadcast_to(sums, (8, 128))

    pltpu.make_async_copy(st_y.at[pl.ds(0, 3)], st_y.at[pl.ds(0, 3)], ars_sem.at[0]).wait()
    pltpu.make_async_copy(st_s.at[pl.ds(0, NSEQ - 1)], st_s.at[pl.ds(0, NSEQ - 1)], ars_sem.at[1]).wait()
    pltpu.make_async_copy(codes_r.at[pl.ds(0, 3)], codes_r.at[pl.ds(0, 3)], csend_sem).wait()
    sent = sendbuf.at[pl.ds(0, NSEQ - 1)]
    pltpu.make_async_copy(sent, sent, send_sem).wait()
    three = out_ref.at[pl.ds(0, 3)]
    pltpu.make_async_copy(three, three, ysend_sem).wait()
    pltpu.make_async_copy(three, three, yrecv_sem).wait()


def finish_kernel(part_ref, stats_ref, out_hbm, loss_ref, share_ref, moved, sem):
    copies = []
    for g in range(128 // ROWS):
        span = pl.ds(ROWS * g, ROWS)
        for b in range(NRES):
            moved[span, b] = jnp.swapaxes(part_ref[b, :, span], 0, 1)
        copies.append(pltpu.make_async_copy(moved.at[span], out_hbm.at[span], sem.at[g]))
        copies[-1].start()
    loss_sum = stats_ref[0, 0]
    mask_count = stats_ref[1, 0]
    loss_ref[0, 0] = loss_sum / (1.0 + mask_count)
    share_ref[0, 0] = mask_count * (1.0 / 1048576)
    for copy in copies:
        copy.wait()


def on_device(alignment, gain_attn, w_proj, w_out, gain_head, w_head, masked, labels):
    vmem = pl.BlockSpec(memory_space=pltpu.VMEM)
    hbm = pl.BlockSpec(memory_space=pltpu.HBM)
    dma = pltpu.SemaphoreType.DMA
    parts, stats = pl.pallas_call(
        exchange_kernel,
        out_shape=(
            jax.ShapeDtypeStruct((NRES, COLS, 128, C), BF),
            jax.ShapeDtypeStruct((8, 128), F32),
        ),
        in_specs=[hbm] * 8,
        out_specs=(vmem, vmem),
        scratch_shapes=[
            pltpu.VMEM((ROWS, S, C), BF),
            pltpu.VMEM((NSEQ, COLS, ROWS, C), BF),
            pltpu.VMEM((COLS, NSEQ, ROWS, C), BF),
            pltpu.VMEM((COLS, S, C), BF),
            pltpu.VMEM((NRES, COLS, 128), jnp.int32),
            pltpu.VMEM((NRES, COLS, 128), jnp.int32),
            pltpu.VMEM((C, 4, C), BF),
            pltpu.VMEM((C, C), BF),
            pltpu.VMEM((3 * C, C), BF),
            pltpu.VMEM((C, C), BF),
            pltpu.VMEM((CLASSES, C), BF),
            pltpu.VMEM((LPAD, C), BF),
            pltpu.VMEM((1, C), F32),
            pltpu.VMEM((1, C), F32),
            pltpu.VMEM((NRES, COLS, 128), jnp.int32),
            pltpu.VMEM((NRES, COLS, 128), jnp.int32),
            pltpu.VMEM((2, HEADS, C, S), BF),
            pltpu.VMEM((2, HEADS, VAUG, S), BF),
            pltpu.VMEM((2, C, S), F32),
            pltpu.VMEM((2, C, S), BF),
            pltpu.VMEM((2, S, C), BF),
            pltpu.VMEM((2, S, S), F32),
            pltpu.VMEM((S, C), BF),
            pltpu.VMEM((S, C), BF),
            pltpu.VMEM((16, 128), F32),
            pltpu.VMEM((NRES, 8, 128), F32),
            pltpu.VMEM((NSEQ, 8, 128), F32),
            dma((4,)), dma((7,)), dma, dma((COLS,)), dma, dma, dma, dma, dma((2,)), dma((2,)),
        ],
        compiler_params=pltpu.CompilerParams(
            collective_id=0, has_side_effects=True, vmem_limit_bytes=VMEM_LIMIT
        ),
        name="exchange",
    )(
        alignment, w_proj, w_out, w_head.T, gain_attn.reshape(1, C), gain_head.reshape(1, C),
        jnp.transpose(masked, (1, 2, 0)), jnp.transpose(labels, (1, 2, 0)),
    )
    smem = pl.BlockSpec(memory_space=pltpu.SMEM)
    updated, loss, share = pl.pallas_call(
        finish_kernel,
        out_shape=(
            jax.ShapeDtypeStruct((128, NRES, COLS, C), BF),
            jax.ShapeDtypeStruct((1, 1), F32),
            jax.ShapeDtypeStruct((1, 1), F32),
        ),
        in_specs=[vmem, smem],
        out_specs=(hbm, smem, smem),
        scratch_shapes=[pltpu.VMEM((128, NRES, COLS, C), BF), dma((128 // ROWS,))],
        compiler_params=pltpu.CompilerParams(vmem_limit_bytes=16 * 2**20),
        name="finish",
    )(parts, stats)
    return updated, loss.reshape(()), share.reshape(())


def solution(mesh):
    split = Mesh(mesh.devices.reshape(4, 4, 2, mesh.shape["res"]), AXES)
    return jax.shard_map(
        on_device,
        mesh=split,
        in_specs=(
            P(SEQ, "res", None, None), P(), P(), P(), P(), P(),
            P("res", None, SEQ), P("res", None, SEQ),
        ),
        out_specs=(P("res", None, SEQ, None), P(), P()),
        check_vma=False,
    )
```

```python
import math

import jax
import jax.numpy as jnp
from jax import lax
from jax.experimental import pallas as pl
from jax.experimental.pallas import tpu as pltpu
from jax.sharding import Mesh
from jax.sharding import PartitionSpec as P

HEADS = 8
HEAD_DIM = 32
CLASSES = 23
C = 256
NSEQ = 32
NRES = 4
ROWS = 16
S = 512
COLS = 16
VAUG = 48
LPAD = 32
AFTER_SLOTS = (0, 0, 1, 2, 3)
BEFORE_SLOTS = (4, 4, 4, 4, 5, 5, 6, 7)
WAIT_SLOT = 4
SEND_SLOT = 2
VMEM_LIMIT = 60 * 2**20
AXES = ("seq_0", "seq_1", "seq_2", "res")
SEQ = AXES[:3]
MESH = pl.DeviceIdType.MESH
BF = jnp.bfloat16
F32 = jnp.float32
QSCALE = HEAD_DIM ** (-0.5) * math.log2(math.e)


def normed_rows(values, gain):
    mean = jnp.mean(values, axis=-1, keepdims=True)
    centred = values - mean
    spread = jnp.mean(centred * centred, axis=-1, keepdims=True)
    return (centred * lax.rsqrt(spread + 1e-05) * gain).astype(BF)


def dot(a, b, dims=((1,), (0,))):
    return lax.dot_general(a, b, (dims, ((), ())), preferred_element_type=F32)


def exchange_kernel(
    align_hbm, w_proj_hbm, w_out_hbm, w_head_hbm, gains_a_hbm, gains_h_hbm, masked_hbm, labels_hbm,
    out_hbm, stats_ref,
    align_v, sendbuf, recv, outbuf, codes, codes_r, w_proj_v, w_k, w_qvg, w_out, w_head_v, w_head,
    gain_attn, gain_head, masked_v, labels_v, qz, va, sg, gated_t, k_nat, sb, nm, hi, acc, st_y, st_s,
    load_sem, small_sem, send_sem, recv_sem, ysend_sem, yrecv_sem, own_sem, code_sem, csend_sem, ar_sem, ars_sem,
):
    x, z, core, y = (lax.axis_index(a) for a in AXES)
    me = (x * 4 + z) * 2 + core

    at_x = [lax.rem(x + d, 4) for d in range(4)]
    at_z = [lax.rem(z + d, 4) for d in range(4)]
    at_core = [core, 1 - core]
    at_y = [lax.rem(y + d, NRES) for d in range(NRES)]

    def seq_device(i):
        return (at_x[i // 8], at_z[i // 2 % 4], at_core[i % 2], y)

    def seq_index(i):
        return (at_x[i // 8] * 4 + at_z[i // 2 % 4]) * 2 + at_core[i % 2]

    def res_device(k):
        return (x, z, core, at_y[k])

    barrier = pltpu.get_barrier_semaphore()

    for i in range(1, NSEQ):
        pl.semaphore_signal(barrier, inc=1, device_id=seq_device(i), device_id_type=MESH)

    for k in range(1, NRES):
        pl.semaphore_signal(barrier, inc=1, device_id=res_device(k), device_id_type=MESH)

    loads = [
        pltpu.make_async_copy(
            align_hbm.at[:, 0, pl.ds(128 * j, 128)], align_v.at[:, pl.ds(128 * j, 128)], load_sem.at[j]
        )
        for j in range(4)
    ]
    small = [
        pltpu.make_async_copy(src, dst, small_sem.at[n])
        for n, (src, dst) in enumerate(
            (
                (masked_hbm, masked_v), (labels_hbm, labels_v), (w_proj_hbm, w_proj_v),
                (w_out_hbm, w_out), (w_head_hbm, w_head_v),
                (gains_a_hbm, gain_attn), (gains_h_hbm, gain_head),
            )
        )
    ]
    for copy in loads + small:
        copy.start()

    for j in range(4):
        loads[j].wait()

        @pl.loop(0, 2)
        def _(g):
            for u in range(4):
                d = 8 * j + 4 * g + u
                block = align_v[:, pl.ds(pl.multiple_of(d * COLS, COLS), COLS)]
                sendbuf[d] = jnp.swapaxes(block, 0, 1)

    recv[:, me] = sendbuf[me]

    for copy in small:
        copy.wait()
    codes[...] = labels_v[...] + 32 * masked_v[...]
    codes_r[y] = codes[y]

    pl.semaphore_wait(barrier, NSEQ - 1 + NRES - 1)

    for k in range(1, NRES):
        pltpu.make_async_remote_copy(
            codes.at[lax.rem(y + k, NRES)], codes_r.at[y], csend_sem, code_sem,
            device_id=res_device(k), device_id_type=MESH,
        ).start()

    @pl.loop(0, COLS)
    def _(c):
        for i in range(1, NSEQ):
            pltpu.make_async_remote_copy(
                sendbuf.at[seq_index(i), c], recv.at[c, me],
                send_sem, recv_sem.at[c], device_id=seq_device(i), device_id_type=MESH,
            ).start()

    for n, i in enumerate((0, 2, 3)):
        w_qvg[pl.ds(C * n, C)] = w_proj_v[:, i].astype(F32).T.astype(BF)
    w_k[...] = w_proj_v[:, 1]
    w_head[...] = jnp.zeros_like(w_head)
    w_head[:CLASSES] = w_head_v[...]
    gated_t[...] = jnp.zeros_like(gated_t)
    acc[...] = jnp.zeros_like(acc)
    for p in range(2):
        qz[p] = jnp.zeros((HEADS, C, S), BF)
        va[p] = jnp.ones((HEADS, VAUG, S), BF)

    pltpu.make_async_copy(codes_r.at[pl.ds(0, 3)], codes_r.at[pl.ds(0, 3)], code_sem).wait()
    count = jnp.sum((codes_r[...] >= 32).astype(F32), axis=0)
    acc[pl.ds(8, 8)] = count[:8] + count[8:]

    def arrived(c):
        span = recv.at[c, pl.ds(0, NSEQ - 1)]
        pltpu.make_async_copy(span, span, recv_sem.at[c]).wait()

    def rows(c, start, n):
        return recv[c, pl.ds(start // ROWS, n // ROWS)].reshape(n, C).astype(F32)

    def before(c, p):
        def norm(start):
            def run():
                nm[pl.ds(start, 128)] = normed_rows(rows(c, start, 128), gain_attn[...])
            return run

        def keys():
            k_nat[p] = dot(nm[...], w_k[...]).astype(BF)

        def queries():
            q_t = (dot(w_qvg[pl.ds(0, C)], nm[...], ((1,), (1,))) * QSCALE).astype(BF)
            for h in range(HEADS):
                part = slice(HEAD_DIM * h, HEAD_DIM * (h + 1))
                qz[p, h, part] = q_t[part]

        def values():
            v_t = dot(w_qvg[pl.ds(C, C)], nm[...], ((1,), (1,))).astype(BF)
            for h in range(HEADS):
                va[p, h, :HEAD_DIM] = v_t[HEAD_DIM * h : HEAD_DIM * (h + 1)]

        def gates():
            g_t = dot(w_qvg[pl.ds(2 * C, C)], nm[...], ((1,), (1,))).astype(BF).astype(F32)
            sg[p] = 0.5 * jnp.tanh(0.5 * g_t) + 0.5

        return [norm(0), norm(128), norm(256), norm(384), keys, queries, values, gates]

    def after(c, p, live):
        def project(start):
            def run():
                added = dot(gated_t[p, :, start : start + 256], w_out[...], ((0,), (0,)))
                outbuf[c, pl.ds(start, 256)] = (rows(c, start, 256) + added).astype(BF)
            return run

        def norm(start):
            def run():
                hi[pl.ds(start, 256)] = normed_rows(outbuf[c, pl.ds(start, 256)].astype(F32), gain_head[...])
            return run

        def loss():
            logits = dot(w_head[...], hi[...], ((1,), (1,)))
            log_total = jnp.log(jnp.sum(jnp.exp(logits[:CLASSES]), axis=0, keepdims=True))
            classes = lax.broadcasted_iota(jnp.int32, (LPAD, 128), 0)
            total = jnp.zeros((1, 128), F32)
            for i in range(NRES):
                lanes = slice(128 * i, 128 * (i + 1))
                code = codes_r[i, pl.ds(c, 1)]
                picked = jnp.sum(
                    jnp.where(classes == (code & 31), logits[:, lanes], 0.0), axis=0, keepdims=True
                )
                total += jnp.where(code >= 32, log_total[:, lanes] - picked, 0.0)
            if live is not None:
                total = jnp.where(live, total, 0.0)
            acc[pl.ds(0, 1)] += total

        return [project(0), project(256), norm(0), norm(256), loss]

    def send_out(c):
        for k in range(1, NRES):
            dst = lax.rem(y + k, NRES)
            pltpu.make_async_remote_copy(
                outbuf.at[c, pl.ds(pl.multiple_of(dst * 128, 128), 128)], out_hbm.at[y, c],
                ysend_sem, yrecv_sem, device_id=res_device(k), device_id_type=MESH,
            ).start()
        pltpu.make_async_copy(
            outbuf.at[c, pl.ds(pl.multiple_of(y * 128, 128), 128)], out_hbm.at[y, c], own_sem
        ).start()

    def score(p, h):
        sb[h % 2] = dot(k_nat[p], qz[p, h])

    def attend(p, h):
        weighted = dot(va[p, h], jnp.exp2(sb[h % 2]).astype(BF))
        part = slice(HEAD_DIM * h, HEAD_DIM * (h + 1))
        inverse = 1.0 / weighted[HEAD_DIM : HEAD_DIM + 1]
        gated_t[p, part] = (weighted[:HEAD_DIM] * inverse * sg[p, part]).astype(BF)

    def body(c, p, following, live):
        slots = [[] for _ in range(HEADS)]
        last = c - 1 if live is None else jnp.maximum(c - 1, 0)
        for slot, piece in zip(AFTER_SLOTS, after(last, 1 - p, live)):
            slots[slot].append(piece)
        if following is not None:
            for slot, piece in zip(BEFORE_SLOTS, before(following, 1 - p)):
                slots[slot].append(piece)
        for h in range(HEADS):
            if h == SEND_SLOT:
                if live is None:
                    send_out(last)
                else:
                    @pl.when(live)
                    def _():
                        send_out(last)
            if h == WAIT_SLOT and following is not None:
                arrived(following)
            if h + 1 < HEADS:
                score(p, h + 1)
            for piece in slots[h]:
                piece()
            if h + 1 == HEADS and following is not None:
                score(1 - p, 0)
            attend(p, h)

    arrived(0)
    for piece in before(0, 0):
        piece()
    score(0, 0)

    @pl.loop(0, COLS // 2 - 1)
    def _(i):
        body(2 * i, 0, 2 * i + 1, i > 0)
        body(2 * i + 1, 1, 2 * i + 2, None)

    body(COLS - 2, 0, COLS - 1, None)
    body(COLS - 1, 1, None, None)
    final = after(COLS - 1, 1, None)
    final[0]()
    final[1]()
    send_out(COLS - 1)
    for piece in final[2:]:
        piece()

    total_count = jnp.sum(acc[pl.ds(8, 8)], axis=0, keepdims=True)
    first = lax.broadcasted_iota(jnp.int32, (8, 128), 0) == 0
    st_s[me] = jnp.where(first, acc[pl.ds(0, 1)], total_count)
    for i in range(1, NSEQ):
        pltpu.make_async_remote_copy(
            st_s.at[me], st_s.at[me], ars_sem.at[0], ar_sem.at[0],
            device_id=seq_device(i), device_id_type=MESH,
        ).start()
    others = st_s.at[pl.ds(0, NSEQ - 1)]
    pltpu.make_async_copy(others, others, ar_sem.at[0]).wait()
    st_y[y] = jnp.sum(st_s[...], axis=0)
    for k in range(1, NRES):
        pltpu.make_async_remote_copy(
            st_y.at[y], st_y.at[y], ars_sem.at[1], ar_sem.at[1],
            device_id=res_device(k), device_id_type=MESH,
        ).start()
    three = st_y.at[pl.ds(0, 3)]
    pltpu.make_async_copy(three, three, ar_sem.at[1]).wait()
    sums = jnp.sum((st_y[0] + st_y[1]) + (st_y[2] + st_y[3]), axis=1, keepdims=True)
    stats_ref[...] = jnp.broadcast_to(sums, (8, 128))

    pltpu.make_async_copy(others, others, ars_sem.at[0]).wait()
    pltpu.make_async_copy(three, three, ars_sem.at[1]).wait()
    pltpu.make_async_copy(codes_r.at[pl.ds(0, 3)], codes_r.at[pl.ds(0, 3)], csend_sem).wait()
    sent = sendbuf.at[pl.ds(0, NSEQ - 1)]
    pltpu.make_async_copy(sent, sent, send_sem).wait()
    pltpu.make_async_copy(out_hbm.at[0], out_hbm.at[0], own_sem).wait()
    three = out_hbm.at[pl.ds(0, 3)]
    pltpu.make_async_copy(three, three, ysend_sem).wait()
    pltpu.make_async_copy(three, three, yrecv_sem).wait()


def finish_kernel(part_hbm, stats_ref, out_hbm, loss_ref, share_ref, part, moved, in_sem, out_sem):
    spans = [pl.ds(ROWS * g, ROWS) for g in range(128 // ROWS)]
    reads = [
        pltpu.make_async_copy(part_hbm.at[:, :, span], part.at[:, :, span], in_sem.at[g])
        for g, span in enumerate(spans)
    ]
    writes = [
        pltpu.make_async_copy(moved.at[span], out_hbm.at[span], out_sem.at[g])
        for g, span in enumerate(spans)
    ]
    for read in reads:
        read.start()
    loss_sum = stats_ref[0, 0]
    mask_count = stats_ref[1, 0]
    loss_ref[0, 0] = loss_sum / (1.0 + mask_count)
    share_ref[0, 0] = mask_count * (1.0 / 1048576)
    for read, write, span in zip(reads, writes, spans):
        read.wait()
        for b in range(NRES):
            moved[span, b] = jnp.swapaxes(part[b, :, span], 0, 1)
        write.start()
    for write in writes:
        write.wait()


def on_device(alignment, gain_attn, w_proj, w_out, gain_head, w_head, masked, labels):
    vmem = pl.BlockSpec(memory_space=pltpu.VMEM)
    hbm = pl.BlockSpec(memory_space=pltpu.HBM)
    dma = pltpu.SemaphoreType.DMA
    parts, stats = pl.pallas_call(
        exchange_kernel,
        out_shape=(
            jax.ShapeDtypeStruct((NRES, COLS, 128, C), BF),
            jax.ShapeDtypeStruct((8, 128), F32),
        ),
        in_specs=[hbm] * 8,
        out_specs=(hbm, vmem),
        scratch_shapes=[
            pltpu.VMEM((ROWS, S, C), BF),
            pltpu.VMEM((NSEQ, COLS, ROWS, C), BF),
            pltpu.VMEM((COLS, NSEQ, ROWS, C), BF),
            pltpu.VMEM((COLS, S, C), BF),
            pltpu.VMEM((NRES, COLS, 128), jnp.int32),
            pltpu.VMEM((NRES, COLS, 128), jnp.int32),
            pltpu.VMEM((C, 4, C), BF),
            pltpu.VMEM((C, C), BF),
            pltpu.VMEM((3 * C, C), BF),
            pltpu.VMEM((C, C), BF),
            pltpu.VMEM((CLASSES, C), BF),
            pltpu.VMEM((LPAD, C), BF),
            pltpu.VMEM((1, C), F32),
            pltpu.VMEM((1, C), F32),
            pltpu.VMEM((NRES, COLS, 128), jnp.int32),
            pltpu.VMEM((NRES, COLS, 128), jnp.int32),
            pltpu.VMEM((2, HEADS, C, S), BF),
            pltpu.VMEM((2, HEADS, VAUG, S), BF),
            pltpu.VMEM((2, C, S), F32),
            pltpu.VMEM((2, C, S), BF),
            pltpu.VMEM((2, S, C), BF),
            pltpu.VMEM((2, S, S), F32),
            pltpu.VMEM((S, C), BF),
            pltpu.VMEM((S, C), BF),
            pltpu.VMEM((16, 128), F32),
            pltpu.VMEM((NRES, 8, 128), F32),
            pltpu.VMEM((NSEQ, 8, 128), F32),
            dma((4,)), dma((7,)), dma, dma((COLS,)), dma, dma, dma, dma, dma, dma((2,)), dma((2,)),
        ],
        compiler_params=pltpu.CompilerParams(
            collective_id=0, has_side_effects=True, vmem_limit_bytes=VMEM_LIMIT
        ),
        name="exchange",
    )(
        alignment, w_proj, w_out, w_head.T, gain_attn.reshape(1, C), gain_head.reshape(1, C),
        jnp.transpose(masked, (1, 2, 0)), jnp.transpose(labels, (1, 2, 0)),
    )
    smem = pl.BlockSpec(memory_space=pltpu.SMEM)
    updated, loss, share = pl.pallas_call(
        finish_kernel,
        out_shape=(
            jax.ShapeDtypeStruct((128, NRES, COLS, C), BF),
            jax.ShapeDtypeStruct((1, 1), F32),
            jax.ShapeDtypeStruct((1, 1), F32),
        ),
        in_specs=[hbm, smem],
        out_specs=(hbm, smem, smem),
        scratch_shapes=[
            pltpu.VMEM((NRES, COLS, 128, C), BF),
            pltpu.VMEM((128, NRES, COLS, C), BF),
            dma((128 // ROWS,)),
            dma((128 // ROWS,)),
        ],
        compiler_params=pltpu.CompilerParams(vmem_limit_bytes=60 * 2**20),
        name="finish",
    )(parts, stats)
    return updated, loss.reshape(()), share.reshape(())


def solution(mesh):
    split = Mesh(mesh.devices.reshape(4, 4, 2, mesh.shape["res"]), AXES)
    return jax.shard_map(
        on_device,
        mesh=split,
        in_specs=(
            P(SEQ, "res", None, None), P(), P(), P(), P(), P(),
            P("res", None, SEQ), P("res", None, SEQ),
        ),
        out_specs=(P("res", None, SEQ, None), P(), P()),
        check_vma=False,
    )
```

```python
import math

import jax
import jax.numpy as jnp
from jax import lax
from jax.experimental import pallas as pl
from jax.experimental.pallas import tpu as pltpu
from jax.sharding import Mesh
from jax.sharding import PartitionSpec as P

HEADS = 8
HEAD_DIM = 32
CLASSES = 23
C = 256
NSEQ = 32
NRES = 4
ROWS = 16
S = 512
COLS = 16
VAUG = 48
LPAD = 32
AFTER_SLOTS = (0, 0, 2, 3, 4)
BEFORE_SLOTS = (5, 5, 5, 5, 6, 6, 6, 7)
WAIT_SLOT = 5
SEND_SLOT = 1
VMEM_LIMIT = 48 * 2**20
AXES = ("seq_0", "seq_1", "seq_2", "res")
SEQ = AXES[:3]
MESH = pl.DeviceIdType.MESH
BF = jnp.bfloat16
F32 = jnp.float32
QSCALE = HEAD_DIM ** (-0.5) * math.log2(math.e)


def normed_rows(values, gain):
    mean = jnp.mean(values, axis=-1, keepdims=True)
    centred = values - mean
    spread = jnp.mean(centred * centred, axis=-1, keepdims=True)
    return (centred * lax.rsqrt(spread + 1e-05) * gain).astype(BF)


def dot(a, b, dims=((1,), (0,))):
    return lax.dot_general(a, b, (dims, ((), ())), preferred_element_type=F32)


def exchange_kernel(
    align_hbm, w_proj_hbm, w_out_hbm, w_head_hbm, gains_a_hbm, gains_h_hbm, masked_hbm, labels_hbm,
    out_hbm, stats_ref,
    align_v, sendbuf, recv, outbuf, codes, codes_r, w_proj_v, w_k, w_qvg, w_out, w_head_v, w_head,
    gain_attn, gain_head, masked_v, labels_v, qz, va, sg, gated_t, k_nat, sb, nm, hi, acc, st_y, st_s,
    load_sem, small_sem, send_sem, recv_sem, ysend_sem, yrecv_sem, code_sem, csend_sem, ar_sem, ars_sem,
):
    x, z, core, y = (lax.axis_index(a) for a in AXES)
    me = (x * 4 + z) * 2 + core

    at_x = [lax.rem(x + d, 4) for d in range(4)]
    at_z = [lax.rem(z + d, 4) for d in range(4)]
    at_core = [core, 1 - core]
    at_y = [lax.rem(y + d, NRES) for d in range(NRES)]

    def seq_device(i):
        return (at_x[i // 8], at_z[i // 2 % 4], at_core[i % 2], y)

    def seq_index(i):
        return (at_x[i // 8] * 4 + at_z[i // 2 % 4]) * 2 + at_core[i % 2]

    def res_device(k):
        return (x, z, core, at_y[k])

    barrier = pltpu.get_barrier_semaphore()

    for i in range(1, NSEQ):
        pl.semaphore_signal(barrier, inc=1, device_id=seq_device(i), device_id_type=MESH)

    for k in range(1, NRES):
        pl.semaphore_signal(barrier, inc=1, device_id=res_device(k), device_id_type=MESH)

    loads = [
        pltpu.make_async_copy(
            align_hbm.at[:, 0, pl.ds(128 * j, 128)], align_v.at[:, pl.ds(128 * j, 128)], load_sem.at[j]
        )
        for j in range(4)
    ]
    small = [
        pltpu.make_async_copy(src, dst, small_sem.at[n])
        for n, (src, dst) in enumerate(
            (
                (masked_hbm, masked_v), (labels_hbm, labels_v), (w_proj_hbm, w_proj_v),
                (w_out_hbm, w_out), (w_head_hbm, w_head_v),
                (gains_a_hbm, gain_attn), (gains_h_hbm, gain_head),
            )
        )
    ]
    for copy in loads + small:
        copy.start()

    for j in range(4):
        loads[j].wait()

        @pl.loop(0, 2)
        def _(g):
            for u in range(4):
                d = 8 * j + 4 * g + u
                block = align_v[:, pl.ds(pl.multiple_of(d * COLS, COLS), COLS)]
                sendbuf[d] = jnp.swapaxes(block, 0, 1)

    recv[:, me] = sendbuf[me]

    for copy in small:
        copy.wait()
    codes[...] = labels_v[...] + 32 * masked_v[...]
    codes_r[y] = codes[y]

    pl.semaphore_wait(barrier, NSEQ - 1 + NRES - 1)

    for k in range(1, NRES):
        pltpu.make_async_remote_copy(
            codes.at[lax.rem(y + k, NRES)], codes_r.at[y], csend_sem, code_sem,
            device_id=res_device(k), device_id_type=MESH,
        ).start()

    @pl.loop(0, COLS)
    def _(c):
        for i in range(1, NSEQ):
            pltpu.make_async_remote_copy(
                sendbuf.at[seq_index(i), c], recv.at[c, me],
                send_sem, recv_sem.at[c], device_id=seq_device(i), device_id_type=MESH,
            ).start()

    for n, i in enumerate((0, 2, 3)):
        w_qvg[pl.ds(C * n, C)] = w_proj_v[:, i].astype(F32).T.astype(BF)
    w_k[...] = w_proj_v[:, 1]
    w_head[...] = jnp.zeros_like(w_head)
    w_head[:CLASSES] = w_head_v[...]
    gated_t[...] = jnp.zeros_like(gated_t)
    acc[...] = jnp.zeros_like(acc)
    for p in range(2):
        qz[p] = jnp.zeros((HEADS, C, S), BF)
        va[p] = jnp.ones((HEADS, VAUG, S), BF)

    pltpu.make_async_copy(codes_r.at[pl.ds(0, 3)], codes_r.at[pl.ds(0, 3)], code_sem).wait()
    count = jnp.sum((codes_r[...] >= 32).astype(F32), axis=0)
    acc[pl.ds(8, 8)] = count[:8] + count[8:]

    def arrived(c):
        span = recv.at[c, pl.ds(0, NSEQ - 1)]
        pltpu.make_async_copy(span, span, recv_sem.at[c]).wait()

    def rows(c, start, n):
        return recv[c, pl.ds(start // ROWS, n // ROWS)].reshape(n, C).astype(F32)

    def before(c, p):
        def norm(start):
            def run():
                nm[pl.ds(start, 128)] = normed_rows(rows(c, start, 128), gain_attn[...])
            return run

        def keys():
            k_nat[p] = dot(nm[...], w_k[...]).astype(BF)

        def queries():
            q_t = (dot(w_qvg[pl.ds(0, C)], nm[...], ((1,), (1,))) * QSCALE).astype(BF)
            for h in range(HEADS):
                part = slice(HEAD_DIM * h, HEAD_DIM * (h + 1))
                qz[p, h, part] = q_t[part]

        def values():
            v_t = dot(w_qvg[pl.ds(C, C)], nm[...], ((1,), (1,))).astype(BF)
            for h in range(HEADS):
                va[p, h, :HEAD_DIM] = v_t[HEAD_DIM * h : HEAD_DIM * (h + 1)]

        def gates():
            g_t = dot(w_qvg[pl.ds(2 * C, C)], nm[...], ((1,), (1,))).astype(BF).astype(F32)
            sg[p] = 0.5 * jnp.tanh(0.5 * g_t) + 0.5

        return [norm(0), norm(128), norm(256), norm(384), keys, queries, values, gates]

    def after(c, p, live):
        def project(start):
            def run():
                added = dot(gated_t[p, :, start : start + 256], w_out[...], ((0,), (0,)))
                outbuf[c, pl.ds(start, 256)] = (rows(c, start, 256) + added).astype(BF)
            return run

        def norm(start):
            def run():
                hi[pl.ds(start, 256)] = normed_rows(outbuf[c, pl.ds(start, 256)].astype(F32), gain_head[...])
            return run

        def loss():
            logits = dot(w_head[...], hi[...], ((1,), (1,)))
            log_total = jnp.log(jnp.sum(jnp.exp(logits[:CLASSES]), axis=0, keepdims=True))
            classes = lax.broadcasted_iota(jnp.int32, (LPAD, 128), 0)
            total = jnp.zeros((1, 128), F32)
            for i in range(NRES):
                lanes = slice(128 * i, 128 * (i + 1))
                code = codes_r[i, pl.ds(c, 1)]
                picked = jnp.sum(
                    jnp.where(classes == (code & 31), logits[:, lanes], 0.0), axis=0, keepdims=True
                )
                total += jnp.where(code >= 32, log_total[:, lanes] - picked, 0.0)
            if live is not None:
                total = jnp.where(live, total, 0.0)
            acc[pl.ds(0, 1)] += total

        return [project(0), project(256), norm(0), norm(256), loss]

    def send_out(c):
        for k in range(1, NRES):
            dst = lax.rem(y + k, NRES)
            pltpu.make_async_remote_copy(
                outbuf.at[c, pl.ds(pl.multiple_of(dst * 128, 128), 128)], out_hbm.at[y, c],
                ysend_sem, yrecv_sem, device_id=res_device(k), device_id_type=MESH,
            ).start()
        out_hbm[y, c] = outbuf[c, pl.ds(pl.multiple_of(y * 128, 128), 128)]

    def score(p, h):
        sb[h % 2] = dot(k_nat[p], qz[p, h])

    def attend(p, h):
        weighted = dot(va[p, h], jnp.exp2(sb[h % 2]).astype(BF))
        part = slice(HEAD_DIM * h, HEAD_DIM * (h + 1))
        inverse = 1.0 / weighted[HEAD_DIM : HEAD_DIM + 1]
        gated_t[p, part] = (weighted[:HEAD_DIM] * inverse * sg[p, part]).astype(BF)

    def body(c, p, following, live):
        slots = [[] for _ in range(HEADS)]
        last = c - 1 if live is None else jnp.maximum(c - 1, 0)
        for slot, piece in zip(AFTER_SLOTS, after(last, 1 - p, live)):
            slots[slot].append(piece)
        if following is not None:
            for slot, piece in zip(BEFORE_SLOTS, before(following, 1 - p)):
                slots[slot].append(piece)
        for h in range(HEADS):
            if h == SEND_SLOT:
                if live is None:
                    send_out(last)
                else:
                    @pl.when(live)
                    def _():
                        send_out(last)
            if h == WAIT_SLOT and following is not None:
                arrived(following)
            if h + 1 < HEADS:
                score(p, h + 1)
            for piece in slots[h]:
                piece()
            if h + 1 == HEADS and following is not None:
                score(1 - p, 0)
            attend(p, h)

    arrived(0)
    for piece in before(0, 0):
        piece()
    score(0, 0)

    @pl.loop(0, COLS // 2 - 1)
    def _(i):
        body(2 * i, 0, 2 * i + 1, i > 0)
        body(2 * i + 1, 1, 2 * i + 2, None)

    body(COLS - 2, 0, COLS - 1, None)
    body(COLS - 1, 1, None, None)
    final = after(COLS - 1, 1, None)
    final[0]()
    final[1]()
    send_out(COLS - 1)
    for piece in final[2:]:
        piece()

    total_count = jnp.sum(acc[pl.ds(8, 8)], axis=0, keepdims=True)
    first = lax.broadcasted_iota(jnp.int32, (8, 128), 0) == 0
    st_s[me] = jnp.where(first, acc[pl.ds(0, 1)], total_count)
    for i in range(1, NSEQ):
        pltpu.make_async_remote_copy(
            st_s.at[me], st_s.at[me], ars_sem.at[0], ar_sem.at[0],
            device_id=seq_device(i), device_id_type=MESH,
        ).start()
    others = st_s.at[pl.ds(0, NSEQ - 1)]
    pltpu.make_async_copy(others, others, ar_sem.at[0]).wait()
    st_y[y] = jnp.sum(st_s[...], axis=0)
    for k in range(1, NRES):
        pltpu.make_async_remote_copy(
            st_y.at[y], st_y.at[y], ars_sem.at[1], ar_sem.at[1],
            device_id=res_device(k), device_id_type=MESH,
        ).start()
    three = st_y.at[pl.ds(0, 3)]
    pltpu.make_async_copy(three, three, ar_sem.at[1]).wait()
    sums = jnp.sum((st_y[0] + st_y[1]) + (st_y[2] + st_y[3]), axis=1, keepdims=True)
    stats_ref[...] = jnp.broadcast_to(sums, (8, 128))

    pltpu.make_async_copy(others, others, ars_sem.at[0]).wait()
    pltpu.make_async_copy(three, three, ars_sem.at[1]).wait()
    pltpu.make_async_copy(codes_r.at[pl.ds(0, 3)], codes_r.at[pl.ds(0, 3)], csend_sem).wait()
    sent = sendbuf.at[pl.ds(0, NSEQ - 1)]
    pltpu.make_async_copy(sent, sent, send_sem).wait()
    three = out_hbm.at[pl.ds(0, 3)]
    pltpu.make_async_copy(three, three, ysend_sem).wait()
    pltpu.make_async_copy(three, three, yrecv_sem).wait()


def finish_kernel(part_ref, stats_ref, out_hbm, loss_ref, share_ref, moved, sem):
    copies = []
    for g in range(128 // ROWS):
        span = pl.ds(ROWS * g, ROWS)
        for b in range(NRES):
            moved[span, b] = jnp.swapaxes(part_ref[b, :, span], 0, 1)
        copies.append(pltpu.make_async_copy(moved.at[span], out_hbm.at[span], sem.at[g]))
        copies[-1].start()
    loss_sum = stats_ref[0, 0]
    mask_count = stats_ref[1, 0]
    loss_ref[0, 0] = loss_sum / (1.0 + mask_count)
    share_ref[0, 0] = mask_count * (1.0 / 1048576)
    for copy in copies:
        copy.wait()


def on_device(alignment, gain_attn, w_proj, w_out, gain_head, w_head, masked, labels):
    vmem = pl.BlockSpec(memory_space=pltpu.VMEM)
    hbm = pl.BlockSpec(memory_space=pltpu.HBM)
    dma = pltpu.SemaphoreType.DMA
    parts, stats = pl.pallas_call(
        exchange_kernel,
        out_shape=(
            jax.ShapeDtypeStruct((NRES, COLS, 128, C), BF),
            jax.ShapeDtypeStruct((8, 128), F32),
        ),
        in_specs=[hbm] * 8,
        out_specs=(vmem, vmem),
        scratch_shapes=[
            pltpu.VMEM((ROWS, S, C), BF),
            pltpu.VMEM((NSEQ, COLS, ROWS, C), BF),
            pltpu.VMEM((COLS, NSEQ, ROWS, C), BF),
            pltpu.VMEM((COLS, S, C), BF),
            pltpu.VMEM((NRES, COLS, 128), jnp.int32),
            pltpu.VMEM((NRES, COLS, 128), jnp.int32),
            pltpu.VMEM((C, 4, C), BF),
            pltpu.VMEM((C, C), BF),
            pltpu.VMEM((3 * C, C), BF),
            pltpu.VMEM((C, C), BF),
            pltpu.VMEM((CLASSES, C), BF),
            pltpu.VMEM((LPAD, C), BF),
            pltpu.VMEM((1, C), F32),
            pltpu.VMEM((1, C), F32),
            pltpu.VMEM((NRES, COLS, 128), jnp.int32),
            pltpu.VMEM((NRES, COLS, 128), jnp.int32),
            pltpu.VMEM((2, HEADS, C, S), BF),
            pltpu.VMEM((2, HEADS, VAUG, S), BF),
            pltpu.VMEM((2, C, S), F32),
            pltpu.VMEM((2, C, S), BF),
            pltpu.VMEM((2, S, C), BF),
            pltpu.VMEM((2, S, S), F32),
            pltpu.VMEM((S, C), BF),
            pltpu.VMEM((S, C), BF),
            pltpu.VMEM((16, 128), F32),
            pltpu.VMEM((NRES, 8, 128), F32),
            pltpu.VMEM((NSEQ, 8, 128), F32),
            dma((4,)), dma((7,)), dma, dma((COLS,)), dma, dma, dma, dma, dma((2,)), dma((2,)),
        ],
        compiler_params=pltpu.CompilerParams(
            collective_id=0, has_side_effects=True, vmem_limit_bytes=VMEM_LIMIT
        ),
        name="exchange",
    )(
        *(
            pltpu.with_memory_space_constraint(array, pltpu.HBM)
            for array in (
                alignment, w_proj, w_out, w_head.T, gain_attn.reshape(1, C), gain_head.reshape(1, C),
                jnp.transpose(masked, (1, 2, 0)), jnp.transpose(labels, (1, 2, 0)),
            )
        )
    )
    smem = pl.BlockSpec(memory_space=pltpu.SMEM)
    updated, loss, share = pl.pallas_call(
        finish_kernel,
        out_shape=(
            jax.ShapeDtypeStruct((128, NRES, COLS, C), BF),
            jax.ShapeDtypeStruct((1, 1), F32),
            jax.ShapeDtypeStruct((1, 1), F32),
        ),
        in_specs=[vmem, smem],
        out_specs=(hbm, smem, smem),
        scratch_shapes=[
            pltpu.VMEM((128, NRES, COLS, C), BF),
            dma((128 // ROWS,)),
        ],
        compiler_params=pltpu.CompilerParams(vmem_limit_bytes=16 * 2**20),
        name="finish",
    )(parts, stats)
    return updated, loss.reshape(()), share.reshape(())


def solution(mesh):
    split = Mesh(mesh.devices.reshape(4, 4, 2, mesh.shape["res"]), AXES)
    return jax.shard_map(
        on_device,
        mesh=split,
        in_specs=(
            P(SEQ, "res", None, None), P(), P(), P(), P(), P(),
            P("res", None, SEQ), P("res", None, SEQ),
        ),
        out_specs=(P("res", None, SEQ, None), P(), P()),
        check_vma=False,
    )
```

```python
import math

import jax
import jax.numpy as jnp
from jax import lax
from jax.experimental import pallas as pl
from jax.experimental.pallas import tpu as pltpu
from jax.sharding import Mesh
from jax.sharding import PartitionSpec as P

HEADS = 8
HEAD_DIM = 32
CLASSES = 23
C = 256
NSEQ = 32
NRES = 4
ROWS = 16
S = 512
COLS = 16
VAUG = 48
LPAD = 32
AFTER_SLOTS = (0, 0, 2, 3, 4)
BEFORE_SLOTS = (5, 5, 5, 5, 6, 6, 6, 7)
WAIT_SLOT = 5
SEND_SLOT = 1
VMEM_LIMIT = 48 * 2**20
AXES = ("seq_0", "seq_1", "seq_2", "res")
SEQ = AXES[:3]
MESH = pl.DeviceIdType.MESH
BF = jnp.bfloat16
F32 = jnp.float32
QSCALE = HEAD_DIM ** (-0.5) * math.log2(math.e)


def hops(i):
    return min(i // 8, 4 - i // 8) + min(i // 2 % 4, 4 - i // 2 % 4)


FAR_FIRST = sorted(range(1, NSEQ), key=hops, reverse=True)


def normed_rows(values, gain):
    mean = jnp.mean(values, axis=-1, keepdims=True)
    centred = values - mean
    spread = jnp.mean(centred * centred, axis=-1, keepdims=True)
    return (centred * lax.rsqrt(spread + 1e-05) * gain).astype(BF)


def dot(a, b, dims=((1,), (0,))):
    return lax.dot_general(a, b, (dims, ((), ())), preferred_element_type=F32)


def exchange_kernel(
    align_hbm, w_proj_hbm, w_out_hbm, w_head_hbm, gains_a_hbm, gains_h_hbm, masked_hbm, labels_hbm,
    out_hbm, stats_ref,
    align_v, sendbuf, recv, outbuf, codes, codes_r, w_proj_v, w_k, w_qvg, w_out, w_head_v, w_head,
    gain_attn, gain_head, masked_v, labels_v, qz, va, sg, gated_t, k_nat, sb, nm, hi, acc, st_y, st_s,
    load_sem, small_sem, send_sem, recv_sem, ysend_sem, yrecv_sem, code_sem, csend_sem, ar_sem, ars_sem,
):
    x, z, core, y = (lax.axis_index(a) for a in AXES)
    me = (x * 4 + z) * 2 + core

    at_x = [lax.rem(x + d, 4) for d in range(4)]
    at_z = [lax.rem(z + d, 4) for d in range(4)]
    at_core = [core, 1 - core]
    at_y = [lax.rem(y + d, NRES) for d in range(NRES)]

    def seq_device(i):
        return (at_x[i // 8], at_z[i // 2 % 4], at_core[i % 2], y)

    def seq_index(i):
        return (at_x[i // 8] * 4 + at_z[i // 2 % 4]) * 2 + at_core[i % 2]

    def res_device(k):
        return (x, z, core, at_y[k])

    barrier = pltpu.get_barrier_semaphore()

    for i in FAR_FIRST:
        pl.semaphore_signal(barrier, inc=1, device_id=seq_device(i), device_id_type=MESH)

    for k in (2, 1, 3):
        pl.semaphore_signal(barrier, inc=1, device_id=res_device(k), device_id_type=MESH)

    loads = [
        pltpu.make_async_copy(
            align_hbm.at[:, 0, pl.ds(128 * j, 128)], align_v.at[:, pl.ds(128 * j, 128)], load_sem.at[j]
        )
        for j in range(4)
    ]
    small = [
        pltpu.make_async_copy(src, dst, small_sem.at[n])
        for n, (src, dst) in enumerate(
            (
                (masked_hbm, masked_v), (labels_hbm, labels_v), (w_proj_hbm, w_proj_v),
                (w_out_hbm, w_out), (w_head_hbm, w_head_v),
                (gains_a_hbm, gain_attn), (gains_h_hbm, gain_head),
            )
        )
    ]
    for copy in loads + small:
        copy.start()

    for j in range(4):
        loads[j].wait()

        @pl.loop(0, 2)
        def _(g):
            for u in range(4):
                d = 8 * j + 4 * g + u
                block = align_v[:, pl.ds(pl.multiple_of(d * COLS, COLS), COLS)]
                sendbuf[d] = jnp.swapaxes(block, 0, 1)

    recv[:, me] = sendbuf[me]

    for copy in small:
        copy.wait()
    codes[...] = labels_v[...] + 32 * masked_v[...]
    codes_r[y] = codes[y]

    pl.semaphore_wait(barrier, NSEQ - 1 + NRES - 1)

    for k in (2, 1, 3):
        pltpu.make_async_remote_copy(
            codes.at[lax.rem(y + k, NRES)], codes_r.at[y], csend_sem, code_sem,
            device_id=res_device(k), device_id_type=MESH,
        ).start()

    @pl.loop(0, COLS)
    def _(c):
        for i in FAR_FIRST:
            pltpu.make_async_remote_copy(
                sendbuf.at[seq_index(i), c], recv.at[c, me],
                send_sem, recv_sem.at[c], device_id=seq_device(i), device_id_type=MESH,
            ).start()

    for n, i in enumerate((0, 2, 3)):
        w_qvg[pl.ds(C * n, C)] = w_proj_v[:, i].astype(F32).T.astype(BF)
    w_k[...] = w_proj_v[:, 1]
    w_head[...] = jnp.zeros_like(w_head)
    w_head[:CLASSES] = w_head_v[...]
    gated_t[...] = jnp.zeros_like(gated_t)
    acc[...] = jnp.zeros_like(acc)
    for p in range(2):
        qz[p] = jnp.zeros((HEADS, C, S), BF)
        va[p] = jnp.ones((HEADS, VAUG, S), BF)

    pltpu.make_async_copy(codes_r.at[pl.ds(0, 3)], codes_r.at[pl.ds(0, 3)], code_sem).wait()
    count = jnp.sum((codes_r[...] >= 32).astype(F32), axis=0)
    acc[pl.ds(8, 8)] = count[:8] + count[8:]

    def arrived(c):
        span = recv.at[c, pl.ds(0, NSEQ - 1)]
        pltpu.make_async_copy(span, span, recv_sem.at[c]).wait()

    def rows(c, start, n):
        return recv[c, pl.ds(start // ROWS, n // ROWS)].reshape(n, C).astype(F32)

    def before(c, p):
        def norm(start):
            def run():
                nm[pl.ds(start, 128)] = normed_rows(rows(c, start, 128), gain_attn[...])
            return run

        def keys():
            k_nat[p] = dot(nm[...], w_k[...]).astype(BF)

        def queries():
            q_t = (dot(w_qvg[pl.ds(0, C)], nm[...], ((1,), (1,))) * QSCALE).astype(BF)
            for h in range(HEADS):
                part = slice(HEAD_DIM * h, HEAD_DIM * (h + 1))
                qz[p, h, part] = q_t[part]

        def values():
            v_t = dot(w_qvg[pl.ds(C, C)], nm[...], ((1,), (1,))).astype(BF)
            for h in range(HEADS):
                va[p, h, :HEAD_DIM] = v_t[HEAD_DIM * h : HEAD_DIM * (h + 1)]

        def gates():
            g_t = dot(w_qvg[pl.ds(2 * C, C)], nm[...], ((1,), (1,))).astype(BF).astype(F32)
            sg[p] = 0.5 * jnp.tanh(0.5 * g_t) + 0.5

        return [norm(0), norm(128), norm(256), norm(384), keys, queries, values, gates]

    def after(c, p, live):
        def project(start):
            def run():
                added = dot(gated_t[p, :, start : start + 256], w_out[...], ((0,), (0,)))
                outbuf[c, pl.ds(start, 256)] = (rows(c, start, 256) + added).astype(BF)
            return run

        def norm(start):
            def run():
                hi[pl.ds(start, 256)] = normed_rows(outbuf[c, pl.ds(start, 256)].astype(F32), gain_head[...])
            return run

        def loss():
            logits = dot(w_head[...], hi[...], ((1,), (1,)))
            log_total = jnp.log(jnp.sum(jnp.exp(logits[:CLASSES]), axis=0, keepdims=True))
            classes = lax.broadcasted_iota(jnp.int32, (LPAD, 128), 0)
            total = jnp.zeros((1, 128), F32)
            for i in range(NRES):
                lanes = slice(128 * i, 128 * (i + 1))
                code = codes_r[i, pl.ds(c, 1)]
                picked = jnp.sum(
                    jnp.where(classes == (code & 31), logits[:, lanes], 0.0), axis=0, keepdims=True
                )
                total += jnp.where(code >= 32, log_total[:, lanes] - picked, 0.0)
            if live is not None:
                total = jnp.where(live, total, 0.0)
            acc[pl.ds(0, 1)] += total

        return [project(0), project(256), norm(0), norm(256), loss]

    def send_out(c):
        for k in (2, 1, 3):
            dst = lax.rem(y + k, NRES)
            pltpu.make_async_remote_copy(
                outbuf.at[c, pl.ds(pl.multiple_of(dst * 128, 128), 128)], out_hbm.at[y, c],
                ysend_sem, yrecv_sem, device_id=res_device(k), device_id_type=MESH,
            ).start()
        out_hbm[y, c] = outbuf[c, pl.ds(pl.multiple_of(y * 128, 128), 128)]

    def score(p, h):
        sb[h % 2] = dot(k_nat[p], qz[p, h])

    def attend(p, h):
        weighted = dot(va[p, h], jnp.exp2(sb[h % 2]).astype(BF))
        part = slice(HEAD_DIM * h, HEAD_DIM * (h + 1))
        inverse = 1.0 / weighted[HEAD_DIM : HEAD_DIM + 1]
        gated_t[p, part] = (weighted[:HEAD_DIM] * inverse * sg[p, part]).astype(BF)

    def body(c, p, following, live):
        slots = [[] for _ in range(HEADS)]
        last = c - 1 if live is None else jnp.maximum(c - 1, 0)
        for slot, piece in zip(AFTER_SLOTS, after(last, 1 - p, live)):
            slots[slot].append(piece)
        if following is not None:
            for slot, piece in zip(BEFORE_SLOTS, before(following, 1 - p)):
                slots[slot].append(piece)
        for h in range(HEADS):
            if h == SEND_SLOT:
                if live is None:
                    send_out(last)
                else:
                    @pl.when(live)
                    def _():
                        send_out(last)
            if h == WAIT_SLOT and following is not None:
                arrived(following)
            if h + 1 < HEADS:
                score(p, h + 1)
            for piece in slots[h]:
                piece()
            if h + 1 == HEADS and following is not None:
                score(1 - p, 0)
            attend(p, h)

    arrived(0)
    for piece in before(0, 0):
        piece()
    score(0, 0)

    @pl.loop(0, COLS // 2 - 1)
    def _(i):
        body(2 * i, 0, 2 * i + 1, i > 0)
        body(2 * i + 1, 1, 2 * i + 2, None)

    body(COLS - 2, 0, COLS - 1, None)
    body(COLS - 1, 1, None, None)
    final = after(COLS - 1, 1, None)
    final[0]()
    final[1]()
    send_out(COLS - 1)
    for piece in final[2:]:
        piece()

    total_count = jnp.sum(acc[pl.ds(8, 8)], axis=0, keepdims=True)
    first = lax.broadcasted_iota(jnp.int32, (8, 128), 0) == 0
    st_s[me] = jnp.where(first, acc[pl.ds(0, 1)], total_count)
    for i in FAR_FIRST:
        pltpu.make_async_remote_copy(
            st_s.at[me], st_s.at[me], ars_sem.at[0], ar_sem.at[0],
            device_id=seq_device(i), device_id_type=MESH,
        ).start()
    others = st_s.at[pl.ds(0, NSEQ - 1)]
    pltpu.make_async_copy(others, others, ar_sem.at[0]).wait()
    st_y[y] = jnp.sum(st_s[...], axis=0)
    for k in (2, 1, 3):
        pltpu.make_async_remote_copy(
            st_y.at[y], st_y.at[y], ars_sem.at[1], ar_sem.at[1],
            device_id=res_device(k), device_id_type=MESH,
        ).start()
    three = st_y.at[pl.ds(0, 3)]
    pltpu.make_async_copy(three, three, ar_sem.at[1]).wait()
    sums = jnp.sum((st_y[0] + st_y[1]) + (st_y[2] + st_y[3]), axis=1, keepdims=True)
    stats_ref[...] = jnp.broadcast_to(sums, (8, 128))

    pltpu.make_async_copy(others, others, ars_sem.at[0]).wait()
    pltpu.make_async_copy(three, three, ars_sem.at[1]).wait()
    pltpu.make_async_copy(codes_r.at[pl.ds(0, 3)], codes_r.at[pl.ds(0, 3)], csend_sem).wait()
    sent = sendbuf.at[pl.ds(0, NSEQ - 1)]
    pltpu.make_async_copy(sent, sent, send_sem).wait()
    three = out_hbm.at[pl.ds(0, 3)]
    pltpu.make_async_copy(three, three, ysend_sem).wait()
    pltpu.make_async_copy(three, three, yrecv_sem).wait()


def finish_kernel(part_ref, stats_ref, out_hbm, loss_ref, share_ref, moved, sem):
    copies = []
    for g in range(128 // ROWS):
        span = pl.ds(ROWS * g, ROWS)
        for b in range(NRES):
            moved[span, b] = jnp.swapaxes(part_ref[b, :, span], 0, 1)
        copies.append(pltpu.make_async_copy(moved.at[span], out_hbm.at[span], sem.at[g]))
        copies[-1].start()
    loss_sum = stats_ref[0, 0]
    mask_count = stats_ref[1, 0]
    loss_ref[0, 0] = loss_sum / (1.0 + mask_count)
    share_ref[0, 0] = mask_count * (1.0 / 1048576)
    for copy in copies:
        copy.wait()


def on_device(alignment, gain_attn, w_proj, w_out, gain_head, w_head, masked, labels):
    vmem = pl.BlockSpec(memory_space=pltpu.VMEM)
    hbm = pl.BlockSpec(memory_space=pltpu.HBM)
    dma = pltpu.SemaphoreType.DMA
    parts, stats = pl.pallas_call(
        exchange_kernel,
        out_shape=(
            jax.ShapeDtypeStruct((NRES, COLS, 128, C), BF),
            jax.ShapeDtypeStruct((8, 128), F32),
        ),
        in_specs=[hbm] * 8,
        out_specs=(vmem, vmem),
        scratch_shapes=[
            pltpu.VMEM((ROWS, S, C), BF),
            pltpu.VMEM((NSEQ, COLS, ROWS, C), BF),
            pltpu.VMEM((COLS, NSEQ, ROWS, C), BF),
            pltpu.VMEM((COLS, S, C), BF),
            pltpu.VMEM((NRES, COLS, 128), jnp.int32),
            pltpu.VMEM((NRES, COLS, 128), jnp.int32),
            pltpu.VMEM((C, 4, C), BF),
            pltpu.VMEM((C, C), BF),
            pltpu.VMEM((3 * C, C), BF),
            pltpu.VMEM((C, C), BF),
            pltpu.VMEM((CLASSES, C), BF),
            pltpu.VMEM((LPAD, C), BF),
            pltpu.VMEM((1, C), F32),
            pltpu.VMEM((1, C), F32),
            pltpu.VMEM((NRES, COLS, 128), jnp.int32),
            pltpu.VMEM((NRES, COLS, 128), jnp.int32),
            pltpu.VMEM((2, HEADS, C, S), BF),
            pltpu.VMEM((2, HEADS, VAUG, S), BF),
            pltpu.VMEM((2, C, S), F32),
            pltpu.VMEM((2, C, S), BF),
            pltpu.VMEM((2, S, C), BF),
            pltpu.VMEM((2, S, S), F32),
            pltpu.VMEM((S, C), BF),
            pltpu.VMEM((S, C), BF),
            pltpu.VMEM((16, 128), F32),
            pltpu.VMEM((NRES, 8, 128), F32),
            pltpu.VMEM((NSEQ, 8, 128), F32),
            dma((4,)), dma((7,)), dma, dma((COLS,)), dma, dma, dma, dma, dma((2,)), dma((2,)),
        ],
        compiler_params=pltpu.CompilerParams(
            collective_id=0, has_side_effects=True, vmem_limit_bytes=VMEM_LIMIT
        ),
        name="exchange",
    )(
        *(
            pltpu.with_memory_space_constraint(array, pltpu.HBM)
            for array in (
                alignment, w_proj, w_out, w_head.T, gain_attn.reshape(1, C), gain_head.reshape(1, C),
                jnp.transpose(masked, (1, 2, 0)), jnp.transpose(labels, (1, 2, 0)),
            )
        )
    )
    smem = pl.BlockSpec(memory_space=pltpu.SMEM)
    updated, loss, share = pl.pallas_call(
        finish_kernel,
        out_shape=(
            jax.ShapeDtypeStruct((128, NRES, COLS, C), BF),
            jax.ShapeDtypeStruct((1, 1), F32),
            jax.ShapeDtypeStruct((1, 1), F32),
        ),
        in_specs=[vmem, smem],
        out_specs=(hbm, smem, smem),
        scratch_shapes=[
            pltpu.VMEM((128, NRES, COLS, C), BF),
            dma((128 // ROWS,)),
        ],
        compiler_params=pltpu.CompilerParams(vmem_limit_bytes=16 * 2**20),
        name="finish",
    )(parts, stats)
    return updated, loss.reshape(()), share.reshape(())


def solution(mesh):
    split = Mesh(mesh.devices.reshape(4, 4, 2, mesh.shape["res"]), AXES)
    return jax.shard_map(
        on_device,
        mesh=split,
        in_specs=(
            P(SEQ, "res", None, None), P(), P(), P(), P(), P(),
            P("res", None, SEQ), P("res", None, SEQ),
        ),
        out_specs=(P("res", None, SEQ, None), P(), P()),
        check_vma=False,
    )
```
